64 devices in a mesh: replica: 4 (over x, y), ep: 16 (over z, core).
Axes of the slice: x: 2, y: 2, z: 8, core: 2. Of those that a mesh axis runs over, the one named last changes fastest.
The devices are a block of a 4x4x8 slice.
Arguments:
- tok_in: bfloat16 [8192, 1536], P(('replica', 'ep')), parts along dimension 0
- routes: int32 [2, 8192, 8], P(None, ('replica', 'ep')), parts along dimension 1
- gate_vals: float32 [2, 8192, 8], P(None, ('replica', 'ep')), parts along dimension 1
- w_gate: bfloat16 [2, 64, 1536, 512], P(None, ('replica', 'ep')), parts along dimension 1
- w_up: bfloat16 [2, 64, 1536, 512], P(None, ('replica', 'ep')), parts along dimension 1
- w_down: bfloat16 [2, 64, 512, 1536], P(None, ('replica', 'ep')), parts along dimension 1
- sh_gate: bfloat16 [2, 1536, 512], replicated
- sh_up: bfloat16 [2, 1536, 512], replicated
- sh_down: bfloat16 [2, 512, 1536], replicated
- old_map: int32 [2, 64], P(None, 'replica'), parts along dimension 1
- move_slot: int32 [2, 16], P(None, 'replica'), parts along dimension 1
- move_expert: int32 [2, 16], P(None, 'replica'), parts along dimension 1
Outputs:
- output 1: bfloat16 [8192, 1536], P(('replica', 'ep')), parts along dimension 0
- output 2: bfloat16 [2, 64, 1536, 512], P(None, ('replica', 'ep')), parts along dimension 1
- output 3: bfloat16 [2, 64, 1536, 512], P(None, ('replica', 'ep')), parts along dimension 1
- output 4: bfloat16 [2, 64, 512, 1536], P(None, ('replica', 'ep')), parts along dimension 1
There are 4 independent parts. The reference program is written for one: setup_inputs(seed, part) draws one part's arguments, and reference() takes and returns one part's arrays. A program takes and returns all parts, laid end to end along the dimension named above; an argument that names none is the same for every part.
All inputs are finite; a program needn't handle non-finite values.
Results may differ from the reference program's by a relative error of at most 0.00277.
Values are sent between devices in bfloat16 or wider.
A program may use at most 768 MiB of HBM per device.

```python
import jax
import jax.numpy as jnp
from jax import lax

HIDDEN = 1536
EXPERT_FF = 512
SHARED_FF = 512
TOP_K = 8
GROUP_DEVS = 16
SLOTS_DEV = 1
TOKENS_DEV = 128
MOVE_COUNT = 4
EXPERTS = 12

SLOT_COUNT = GROUP_DEVS * SLOTS_DEV
TOKEN_COUNT = GROUP_DEVS * TOKENS_DEV
SCORE_RANGE = 2 ** 10
HOT_BONUS = 2 ** 9
COVER_BONUS = 2 ** 12


def draw_layout(rng_key):
    perm_key, extra_key, place_key = jax.random.split(rng_key, 3)
    expert_perm = jax.random.permutation(perm_key, EXPERTS).astype(jnp.int32)
    extra_slot = jax.random.randint(extra_key, (SLOT_COUNT - EXPERTS,), 0, EXPERTS, dtype=jnp.int32)
    canon_old = jnp.concatenate([expert_perm, extra_slot])
    cycled = jnp.concatenate([expert_perm[1:MOVE_COUNT], expert_perm[:1]])
    slot_perm = jax.random.permutation(place_key, SLOT_COUNT).astype(jnp.int32)
    old_map = canon_old[slot_perm]
    slot_of_canon = jnp.argsort(slot_perm).astype(jnp.int32)
    return old_map, slot_of_canon[:MOVE_COUNT], cycled, expert_perm[:MOVE_COUNT]


def draw_routes(rng_key, hot_ids):
    score_key, offset_key = jax.random.split(rng_key)
    score_int = jax.random.randint(score_key, (TOKEN_COUNT, EXPERTS), 0, SCORE_RANGE, dtype=jnp.int32)
    expert_ids = jnp.arange(EXPERTS, dtype=jnp.int32)
    is_hot = jnp.any(expert_ids[:, None] == hot_ids[None, :], axis=1).astype(jnp.int32)
    offset = jax.random.randint(offset_key, (), 0, EXPERTS, dtype=jnp.int32)
    token_ids = jnp.arange(TOKEN_COUNT, dtype=jnp.int32)
    cover_mask = ((token_ids[:, None] + offset) % EXPERTS == expert_ids[None, :]).astype(jnp.int32)
    total_score = score_int + HOT_BONUS * is_hot[None, :] + COVER_BONUS * cover_mask
    picked = lax.top_k(total_score * EXPERTS + expert_ids[None, :], TOP_K)[1]
    return picked.astype(jnp.int32)


def place_slots(expert_w, slot_map):
    return jnp.take(expert_w, slot_map, axis=0)


def setup_inputs(seed: int = 0, part: int = 0) -> dict:
    base_key = jax.random.key(seed)
    part_key = jax.random.fold_in(base_key, part)
    draw_keys = jax.random.split(part_key, 7)
    shared_keys = jax.random.split(jax.random.key(seed + 1), 3)
    old_map, move_slot, move_expert, hot_ids = jax.vmap(draw_layout)(jax.random.split(draw_keys[0], 2))
    routes = jax.vmap(draw_routes)(jax.random.split(draw_keys[1], 2), hot_ids)
    gate_vals = (0.5 + jax.random.uniform(draw_keys[2], (2, TOKEN_COUNT, TOP_K))) / TOP_K ** 0.5
    tok_in = jax.random.normal(draw_keys[3], (TOKEN_COUNT, HIDDEN)).astype(jnp.bfloat16)
    gate_e = (jax.random.normal(draw_keys[4], (2, EXPERTS, HIDDEN, EXPERT_FF)) * HIDDEN ** -0.5).astype(jnp.bfloat16)
    up_e = (jax.random.normal(draw_keys[5], (2, EXPERTS, HIDDEN, EXPERT_FF)) * HIDDEN ** -0.5).astype(jnp.bfloat16)
    down_e = (jax.random.normal(draw_keys[6], (2, EXPERTS, EXPERT_FF, HIDDEN)) * EXPERT_FF ** -0.5).astype(jnp.bfloat16)
    sh_gate = (jax.random.normal(shared_keys[0], (2, HIDDEN, SHARED_FF)) * HIDDEN ** -0.5).astype(jnp.bfloat16)
    sh_up = (jax.random.normal(shared_keys[1], (2, HIDDEN, SHARED_FF)) * HIDDEN ** -0.5).astype(jnp.bfloat16)
    sh_down = (jax.random.normal(shared_keys[2], (2, SHARED_FF, HIDDEN)) * SHARED_FF ** -0.5).astype(jnp.bfloat16)
    return {
        'tok_in': tok_in,
        'routes': routes,
        'gate_vals': gate_vals,
        'w_gate': jax.vmap(place_slots)(gate_e, old_map),
        'w_up': jax.vmap(place_slots)(up_e, old_map),
        'w_down': jax.vmap(place_slots)(down_e, old_map),
        'sh_gate': sh_gate,
        'sh_up': sh_up,
        'sh_down': sh_down,
        'old_map': old_map,
        'move_slot': move_slot,
        'move_expert': move_expert,
    }


def first_holder(slot_map, wanted):
    slot_ids = jnp.arange(SLOT_COUNT, dtype=jnp.int32)
    hit_mask = slot_map[None, :] == wanted[:, None]
    return jnp.min(jnp.where(hit_mask, slot_ids[None, :], SLOT_COUNT), axis=1)


def swiglu(hidden, w_gate, w_up, w_down):
    gate_proj = jnp.dot(hidden, w_gate, preferred_element_type=jnp.float32)
    up_proj = jnp.dot(hidden, w_up, preferred_element_type=jnp.float32)
    inner_act = (jax.nn.silu(gate_proj) * up_proj).astype(jnp.bfloat16)
    return jnp.dot(inner_act, w_down, preferred_element_type=jnp.float32)


def moe_layer(hidden, route_ids, gate_w, w_gate, w_up, w_down, sh_gate, sh_up, sh_down, slot_map):
    expert_ids = jnp.arange(EXPERTS, dtype=jnp.int32)
    holders = first_holder(slot_map, expert_ids)

    def add_expert(running, expert_idx):
        holder_slot = holders[expert_idx]
        expert_out = swiglu(hidden, w_gate[holder_slot], w_up[holder_slot], w_down[holder_slot])
        gate_col = jnp.sum(jnp.where(route_ids == expert_idx, gate_w, 0.0), axis=1)
        return running + gate_col[:, None] * expert_out, None

    start_acc = hidden.astype(jnp.float32) + swiglu(hidden, sh_gate, sh_up, sh_down)
    total_out = lax.scan(add_expert, start_acc, expert_ids)[0]
    return total_out.astype(jnp.bfloat16)


def reference(tok_in, routes, gate_vals, w_gate, w_up, w_down, sh_gate, sh_up, sh_down, old_map, move_slot, move_expert):
    hidden = tok_in
    new_sets = []
    for layer_idx in range(2):
        hidden = moe_layer(hidden, routes[layer_idx], gate_vals[layer_idx], w_gate[layer_idx], w_up[layer_idx], w_down[layer_idx], sh_gate[layer_idx], sh_up[layer_idx], sh_down[layer_idx], old_map[layer_idx])
        new_map = old_map[layer_idx].at[move_slot[layer_idx]].set(move_expert[layer_idx])
        source = first_holder(old_map[layer_idx], new_map)
        new_sets.append((jnp.take(w_gate[layer_idx], source, axis=0), jnp.take(w_up[layer_idx], source, axis=0), jnp.take(w_down[layer_idx], source, axis=0)))
    new_gate = jnp.stack([new_sets[0][0], new_sets[1][0]])
    new_up = jnp.stack([new_sets[0][1], new_sets[1][1]])
    new_down = jnp.stack([new_sets[0][2], new_sets[1][2]])
    return (hidden, new_gate, new_up, new_down)
```

```python
import functools
import jax
import jax.numpy as jnp
from jax import lax
from jax.experimental import pallas as pl
from jax.experimental.pallas import tpu as pltpu
from jax.sharding import PartitionSpec as P

TOKEN_AXES = ('replica', 'ep')
MESH = pl.DeviceIdType.MESH
ANY = pl.BlockSpec(memory_space=pl.ANY)
VM = pl.BlockSpec(memory_space=pltpu.VMEM)
SM = pl.BlockSpec(memory_space=pltpu.SMEM)

CHUNK = 16
HOP_LAG = 5
OUT_LAG = 2
SLOTS = 48
PARTS = 4
FAST_BUSES, FAST_REACH = (4, 5), 6


def sel(pred, a, b):
    return lax.select_n(pred, b, a)


def plan_kernel(chips, me_ref, old_ref, ms_ref, mx_ref, fast_in, fast_out, slow_in, slow_out, level_ref, serve_ref):
    layers, slots = old_ref.shape
    moves = ms_ref.shape[1]
    full = layers * moves
    me = me_ref[0]
    my_core, my_chip = me & 1, lax.shift_right_logical(me, 1)

    def wrap(x):
        return x & (chips - 1) if chips & (chips - 1) == 0 else lax.rem(x, chips)

    for layer in range(layers):
        held = [old_ref[layer, q] for q in range(slots)]
        for q in range(slots):
            again = jnp.bool_(False)
            for p in range(q):
                again = again | (held[p] == held[q])
            serve_ref[layer, q] = jnp.where(again, -1, held[q])
    for ref in (fast_in, slow_in):
        for a in range(ref.shape[0]):
            for b in range(ref.shape[1]):
                ref[a, b] = 0
    for ref in (fast_out, slow_out):
        for a in range(ref.shape[0]):
            ref[a] = 0
    ring = (1 << chips) - 1

    def arc(start, dist, sign):
        run = lax.shift_left(1, dist) - 1
        low = start if sign > 0 else wrap(start - dist + 1 + chips)
        turned = lax.shift_left(run, low)
        return (turned | lax.shift_right_logical(turned, chips)) & ring

    routes = []
    for n in range(full):
        layer, i = divmod(n, moves)
        want, tgt = mx_ref[layer, i], ms_ref[layer, i]
        tgt_chip = lax.shift_right_logical(tgt, 1)
        best_key, src = jnp.int32(1 << 20), jnp.int32(0)
        for q in range(slots):
            fwd = wrap(tgt_chip - q // 2 + chips)
            key = jnp.minimum(fwd, chips - fwd)
            better = (old_ref[layer, q] == want) & (key < best_key)
            best_key = jnp.where(better, key, best_key)
            src = jnp.where(better, q, src)
        start = lax.shift_right_logical(src, 1)
        fwd = wrap(tgt_chip - start + chips)
        dists = (fwd, chips - fwd)
        bits = (arc(start, dists[0], 1), arc(start, dists[1], -1))
        routes.append((src, tgt, fwd == 0, dists, bits))

    def attempt(order, buses):
        used = [[jnp.int32(0)] * buses for _ in range(2)]
        picks, fits = {}, jnp.bool_(True)
        for half in range(2):
            for n in order:
                _, _, near, dists, bits = routes[n]
                found = []
                for lane in range(2):
                    bus = jnp.int32(buses)
                    for b in reversed(range(buses)):
                        bus = jnp.where((used[lane][b] & bits[lane]) == 0, b, bus)
                    found.append(jnp.where(dists[lane] > FAST_REACH, buses, bus))
                second = found[1] * 2 * chips + dists[1] < found[0] * 2 * chips + dists[0]
                bus = jnp.where(second, found[1], found[0])
                fits = fits & (near | (bus < buses))
                for lane in range(2):
                    mine = jnp.logical_not(near) & (second if lane == 1 else jnp.logical_not(second))
                    for b in range(buses):
                        used[lane][b] = used[lane][b] | jnp.where(mine & (bus == b), bits[lane], 0)
                picks[n, half] = (second.astype(jnp.int32), bus)
        return picks, fits

    evens, odds = list(range(0, full, 2)), list(range(1, full, 2))
    straight = list(range(full))
    orders = [straight, straight[::-1], straight[full // 2:] + straight[:full // 2], odds + evens]
    picks, level = attempt(straight, FAST_BUSES[1])
    level = jnp.where(level, 1, 2)
    for order in orders:
        other, fits = attempt(order, FAST_BUSES[0])
        for key in picks:
            picks[key] = tuple(jnp.where(fits, new, old) for new, old in zip(other[key], picks[key]))
        level = jnp.where(fits, 0, level)
    level_ref[...] = jnp.full(level_ref.shape, level, jnp.int32)

    def emit(in_ref, out_ref, lane, bus, dist, n, half, on):
        src, tgt = routes[n][:2]
        piece = 2 * (n // moves) + half

        @pl.when(on & (my_core == lane) & (my_chip == lax.shift_right_logical(src, 1)))
        def _():
            in_ref[bus, 0] = 1
            in_ref[bus, 1] = ((src & 1) != my_core).astype(jnp.int32)
            in_ref[bus, 2] = piece
            in_ref[bus, 3] = dist

        @pl.when(on & (tgt == me))
        def _():
            out_ref[piece] = jnp.where(my_core == lane, 2 + bus, 2 + full + bus)

    for n in range(full):
        src, tgt, near, dists, _ = routes[n]
        for half in range(2):
            lane, bus = picks[n, half]
            ok = jnp.logical_not(near) & (bus < FAST_BUSES[1])
            emit(fast_in, fast_out, lane, bus, jnp.where(lane == 1, dists[1], dists[0]), n, half, ok)
            emit(slow_in, slow_out, half, n, dists[half], n, half, jnp.logical_not(near))

            @pl.when(near & (tgt == me))
            def _():
                fast_out[2 * (n // moves) + half] = 1
                slow_out[2 * (n // moves) + half] = 1


def plan_moves(me, old_map, move_slot, move_expert, chips):
    layers, moves = move_slot.shape
    full = layers * moves
    i32 = jnp.int32
    return pl.pallas_call(
        functools.partial(plan_kernel, chips),
        out_shape=(jax.ShapeDtypeStruct((FAST_BUSES[1], 4), i32), jax.ShapeDtypeStruct((2 * layers,), i32),
                   jax.ShapeDtypeStruct((full, 4), i32), jax.ShapeDtypeStruct((2 * layers,), i32),
                   jax.ShapeDtypeStruct((8, 128), i32), jax.ShapeDtypeStruct(old_map.shape, i32)),
        in_specs=[SM] * 4, out_specs=(SM,) * 4 + (VM, SM),
    )(me, old_map, move_slot, move_expert)


def bus_kernel(axis_size, buses, reach, full, in_tab, out_tab, wg, wu, wd, ng, nu, nd, *scratch):
    owns, pars = scratch[:PARTS], scratch[PARTS:2 * PARTS]
    recv, send, prx, load_sem, dsend, drecv, send_sem, recv_sem, push_sem, prx_sem = scratch[2 * PARTS:]
    me = lax.axis_index('ep')
    core = lax.rem(me, 2)
    step_dir = 2 - 4 * core
    nxt = lax.rem(me + step_dir + axis_size, axis_size)
    prv = lax.rem(me - step_dir + axis_size, axis_size)
    mate = me + 1 - 2 * core
    layers, tall, width = wg.shape[0], wg.shape[1], wg.shape[3]
    low, blocks = wd.shape[1], wd.shape[3] // width
    half_chunks = (2 * tall + blocks * low) // 2
    span = half_chunks // PARTS

    def pieces(part, g, u, d):
        out = []
        for layer in range(layers):
            areas = [(g.at[layer], 0, tall), (u.at[layer], tall, tall)]
            areas += [(d.at[layer, :, :, pl.ds(n * width, width)], 2 * tall + n * low, low) for n in range(blocks)]
            for half in range(2):
                lo = half * half_chunks + part * span
                for ref, at, size in areas:
                    first, last = max(lo, at), min(lo + span, at + size)
                    if first < last:
                        out.append((ref.at[pl.ds(first - at, last - first)], (2 * layer + half) * span + first - lo, last - first))
        return out

    def local_copies(part, refs, out):
        copies = []
        for n, (ref, at, size) in enumerate(pieces(part, *refs)):
            here = owns[part].at[pl.ds(at, size)]
            copies.append(pltpu.make_async_copy(*((here, ref) if out else (ref, here)), load_sem.at[part, n]))
        return copies

    def share(part):
        return pltpu.make_async_remote_copy(owns[part], pars[part], dsend.at[part], drecv.at[part],
                                            device_id={'ep': mate}, device_id_type=MESH)

    def ring_copy(slot):
        return pltpu.make_async_remote_copy(send.at[slot], recv.at[slot], send_sem.at[slot], recv_sem.at[slot],
                                            device_id={'ep': nxt}, device_id_type=MESH)

    def push_copy(slot):
        return pltpu.make_async_remote_copy(recv.at[slot], prx.at[slot], push_sem.at[slot], prx_sem.at[slot],
                                            device_id={'ep': mate}, device_id_type=MESH)

    for copy in local_copies(0, (wg, wu, wd), False):
        copy.start()
    barrier = pltpu.get_barrier_semaphore()
    for peer in (nxt, prv, mate):
        pl.semaphore_signal(barrier, inc=1, device_id={'ep': peer}, device_id_type=MESH)
    pl.semaphore_wait(barrier, 3)
    for part in range(PARTS):
        for copy in local_copies(part, (wg, wu, wd), False):
            copy.wait()
        share(part).start()
        if part == 0:
            for later in range(1, PARTS):
                for copy in local_copies(later, (wg, wu, wd), False):
                    copy.start()

    sends = half_chunks + (reach - 1) * HOP_LAG
    first_out = reach * HOP_LAG
    first_store = first_out + OUT_LAG
    total = first_store + half_chunks
    edges = {0, HOP_LAG, sends, sends + HOP_LAG, first_out, first_out + half_chunks, total}
    edges |= {p * span for p in range(PARTS + 1)} | {first_store + p * span for p in range(PARTS)}
    edges = sorted(edges)

    for begin, end in zip(edges[:-1], edges[1:]):
        lead = min(begin // span, PARTS - 1)
        if begin % span == 0 and begin < half_chunks:
            share(lead).wait()
        done = (begin - first_store) // span
        if begin >= first_store and (begin - first_store) % span == 0 and done > 0:
            for copy in local_copies(done - 1, (ng, nu, nd), True):
                copy.start()

        def step(t, carry, begin=begin, lead=lead, done=done):
            slot = lax.rem(t, SLOTS)
            old_slot = lax.rem(t - HOP_LAG + SLOTS, SLOTS)
            if HOP_LAG <= begin < sends + HOP_LAG:
                ring_copy(old_slot).wait()
            if begin < sends:
                for j in range(buses):
                    pick = t - (reach - in_tab[j, 3]) * HOP_LAG
                    at = in_tab[j, 2] * span
                    late = at + jnp.minimum(jnp.maximum(pick - lead * span, 0), span - 1)
                    mine, theirs = owns[lead][late], pars[lead][late]
                    if lead > 0:
                        early = at + jnp.minimum(jnp.maximum(pick - (lead - 1) * span, 0), span - 1)
                        fresh = pick >= lead * span
                        mine = sel(fresh, mine, owns[lead - 1][early])
                        theirs = sel(fresh, theirs, pars[lead - 1][early])
                    value = sel(in_tab[j, 1] != 0, theirs, mine)
                    if begin >= HOP_LAG:
                        value = sel(in_tab[j, 0] != 0, value, recv[old_slot, j])
                    send[slot, j] = value
                ring_copy(slot).start()
            if first_out <= begin < first_out + half_chunks:
                push_copy(old_slot).start()
            if begin >= first_store:
                k = t - first_store - done * span
                src = lax.rem(t - OUT_LAG - HOP_LAG + SLOTS, SLOTS)
                push_copy(src).wait()
                for piece in range(2 * layers):
                    code = out_tab[piece]
                    at = piece * span + k
                    value = sel(code == 1, pars[done][at], owns[done][at])
                    for j in range(buses):
                        value = sel(code == 2 + j, recv[src, j], value)
                        value = sel(code == 2 + full + j, prx[src, j], value)
                    owns[done][at] = value
            return carry

        lax.fori_loop(begin, end, step, 0)

    for copy in local_copies(PARTS - 1, (ng, nu, nd), True):
        copy.start()
    for part in range(PARTS):
        for copy in local_copies(part, (ng, nu, nd), True):
            copy.wait()


def move_weights(axis_size, buses, reach, full, cid, in_tab, out_tab, *weights):
    cut = [w.reshape(w.shape[0], w.shape[2] // CHUNK, CHUNK, w.shape[3]) for w in weights]
    layers, tall, _, width = cut[0].shape
    low, blocks = cut[2].shape[1], cut[2].shape[3] // width
    bf16 = jnp.bfloat16
    dma = pltpu.SemaphoreType.DMA
    ring = pltpu.VMEM((SLOTS, buses, CHUNK, width), bf16)
    part = pltpu.VMEM((layers * (2 * tall + blocks * low) // PARTS, CHUNK, width), bf16)
    out = pl.pallas_call(
        functools.partial(bus_kernel, axis_size, buses, reach, full),
        out_shape=tuple(jax.ShapeDtypeStruct(w.shape, bf16) for w in cut),
        in_specs=[SM, SM, ANY, ANY, ANY], out_specs=(ANY,) * 3,
        scratch_shapes=[part] * (2 * PARTS) + [ring, ring, ring,
                        dma((PARTS, 4 * layers)), dma((PARTS,)), dma((PARTS,)),
                        dma((SLOTS,)), dma((SLOTS,)), dma((SLOTS,)), dma((SLOTS,))],
        compiler_params=pltpu.CompilerParams(collective_id=cid, has_side_effects=True, vmem_limit_bytes=(42 if buses > 5 else 34) * 1024 * 1024),
    )(in_tab, out_tab, *cut)
    return tuple(n.reshape(w.shape) for n, w in zip(out, weights))


def new_layout(axis_size, plan, level, *weights):
    fast_in, fast_out, slow_in, slow_out = plan[:4]
    full = slow_in.shape[0]

    def fast(buses, cid):
        return lambda *w: move_weights(axis_size, buses, FAST_REACH, full, cid, fast_in, fast_out, *w)

    def slow(*w):
        return move_weights(axis_size, full, axis_size // 2 - 1, full, 3, slow_in, slow_out, *w)

    return lax.switch(level, (fast(FAST_BUSES[0], 1), fast(FAST_BUSES[1], 2), slow), *weights)


SUBS = 2


def token_kernel(axis_size, groups, tok, gt, flag, wg, wu, wd, sg, su, sd, out, any_flag,
                 xb, rs, pp, pst, first, home, gbuf, fbuf, eg, eu, ed, hg, hu, hd,
                 w_sem, s_sem, g_send, g_recv, x_send, x_recv, m_send, m_recv, p_send, p_recv, r_send, r_recv, f_send, f_recv):
    me = lax.axis_index('ep')
    core, chip = lax.rem(me, 2), lax.div(me, 2)
    chips = axis_size // 2
    step_dir = 2 - 4 * core
    nxt = lax.rem(me + step_dir + axis_size, axis_size)
    mate = me + 1 - 2 * core
    layers = wg.shape[0]
    rows, width = tok.shape
    hops = chips - 1
    cols = wg.shape[2]

    def shared_loads(layer):
        return [pltpu.make_async_copy(a.at[layer], b, s_sem.at[n]) for n, (a, b) in enumerate(((sg, hg), (su, hu), (sd, hd)))]

    def expert_loads(layer):
        return [pltpu.make_async_copy(a.at[layer], b.at[layer], w_sem.at[3 * layer + n])
                for n, (a, b) in enumerate(((wg, eg), (wu, eu), (wd, ed)))]

    for copy in shared_loads(0) + expert_loads(0):
        copy.start()
    barrier = pltpu.get_barrier_semaphore()
    for off in range(1, axis_size):
        pl.semaphore_signal(barrier, inc=1, device_id={'ep': lax.rem(me + off, axis_size)}, device_id_type=MESH)
    group = lax.axis_index('replica')
    for off in range(1, groups):
        pl.semaphore_signal(barrier, inc=1, device_id={'replica': lax.rem(group + off, groups)}, device_id_type=MESH)
    pl.semaphore_wait(barrier, axis_size + groups - 2)

    def token_copy(src_slot, dst_slot, sub):
        piece = pl.ds(sub * (rows // SUBS), rows // SUBS)
        return pltpu.make_async_remote_copy(xb.at[src_slot, core, piece], xb.at[dst_slot, core, piece],
                                            x_send.at[dst_slot, sub], x_recv.at[dst_slot, sub],
                                            device_id={'ep': nxt}, device_id_type=MESH)

    def mate_copy(slot):
        return pltpu.make_async_remote_copy(xb.at[slot, core], xb.at[slot, core], m_send.at[slot], m_recv.at[slot],
                                            device_id={'ep': mate}, device_id_type=MESH)

    def mate_arrival(slot):
        other = 1 - core
        return pltpu.make_async_remote_copy(xb.at[slot, other], xb.at[slot, other], m_send.at[slot], m_recv.at[slot],
                                            device_id={'ep': mate}, device_id_type=MESH)

    def part_copy(stage, slot, c):
        blk = pl.ds(c * cols, cols)
        return pltpu.make_async_remote_copy(pst.at[stage, 1 - core, :, blk], pp.at[slot, :, blk], p_send.at[stage, c], p_recv.at[slot, c],
                                            device_id={'ep': mate}, device_id_type=MESH)

    def sum_copy(src, at, slot, sub):
        piece = pl.ds(sub * (rows // SUBS), rows // SUBS)
        return pltpu.make_async_remote_copy(src.at[at, piece], rs.at[slot, piece], r_send.at[slot, sub], r_recv.at[slot, sub],
                                            device_id={'ep': nxt}, device_id_type=MESH)

    xb[hops, core] = tok[...]
    for sub in range(SUBS):
        token_copy(hops, 0, sub).start()
    mate_copy(hops).start()

    def gate_copy(off):
        peer = lax.rem(me + off, axis_size)
        return pltpu.make_async_remote_copy(gt.at[peer], gbuf.at[me], g_send.at[off], g_recv.at[off],
                                            device_id={'ep': peer}, device_id_type=MESH)

    def gate_arrival(off):
        peer = lax.rem(me - off + axis_size, axis_size)
        return pltpu.make_async_remote_copy(gt.at[peer], gbuf.at[peer], g_send.at[off], g_recv.at[off],
                                            device_id={'ep': peer}, device_id_type=MESH)

    for off in range(1, axis_size):
        gate_copy(off).start()
    gbuf[me] = gt[me]

    def flag_copy(off):
        peer = lax.rem(group + off, groups)
        return pltpu.make_async_remote_copy(flag, fbuf.at[off], f_send.at[off], f_recv.at[off],
                                            device_id={'replica': peer}, device_id_type=MESH)

    for off in range(1, groups):
        flag_copy(off).start()
    fbuf[0] = flag[...]

    def inner(x, w_gate, w_up):
        gate_proj = jnp.dot(x, w_gate, preferred_element_type=jnp.float32)
        up_proj = jnp.dot(x, w_up, preferred_element_type=jnp.float32)
        return (jax.nn.silu(gate_proj) * up_proj).astype(jnp.bfloat16)

    def spread(src, layer):
        row = gbuf[src, pl.ds(layer, 1), :]
        return jnp.broadcast_to(row, (rows, rows)).T

    for layer in range(layers):
        base = layer * chips
        rbase = layer * hops
        own = base + hops
        for copy in shared_loads(layer):
            copy.wait()
        mine = xb[own, core]
        act = inner(mine, hg[...], hu[...])
        for c in range(width // cols):
            blk = pl.ds(c * cols, cols)
            home[:, blk] = xb[own, core, :, blk].astype(jnp.float32) + jnp.dot(act, hd[:, blk], preferred_element_type=jnp.float32)
        if layer + 1 < layers:
            for copy in shared_loads(layer + 1):
                copy.start()
        def relay(slot, onward):
            for sub in range(SUBS):
                token_copy(slot, slot, sub).wait_recv()

                @pl.when(onward)
                def _():
                    token_copy(slot, slot + 1, sub).start()
            mate_copy(slot).start()

        def partial(s):
            slot, stage = base + s, lax.rem(s, 2)
            mate_arrival(slot).wait_recv()

            @pl.when(s >= 2)
            def _():
                for c in range(width // cols):
                    part_copy(stage, slot, c).wait_send()
            x = xb[slot].reshape(2 * rows, width)
            act = inner(x, eg[layer], eu[layer])

            @pl.when(s + 1 < hops)
            def _():
                relay(slot + 1, s + 2 < hops)
            src_a = 2 * lax.rem(chip - 1 - s + 2 * chips, chips)
            src_b = 2 * lax.rem(chip + 1 + s, chips) + 1
            scale = jnp.concatenate([spread(src_a, layer), spread(src_b, layer)], axis=0)
            scale = jnp.concatenate([scale] * (cols // rows), axis=1)
            for c in range(width // cols):
                blk = pl.ds(c * cols, cols)
                y = jnp.dot(act, ed[layer, :, blk], preferred_element_type=jnp.float32) * scale
                pst[stage, 0, :, blk] = y[:rows]
                pst[stage, 1, :, blk] = y[rows:]
                part_copy(stage, slot, c).start()

        def step(s, carry):
            @pl.when(s >= 0)
            def _():
                slot, stage = base + s, lax.rem(s, 2)
                for c in range(width // cols):
                    part_copy(stage, slot, c).wait_recv()
                for sub in range(SUBS):
                    piece = pl.ds(sub * (rows // SUBS), rows // SUBS)

                    @pl.when(s == 0)
                    def _():
                        first[layer, piece] = pst[stage, core, piece] + pp[slot, piece]
                        sum_copy(first, layer, rbase, sub).start()

                    @pl.when(s > 0)
                    def _():
                        sum_copy(rs, 0, rbase + s - 1, sub).wait_recv()

                    @pl.when((s > 0) & (s < hops))
                    def _():
                        at = rbase + s - 1
                        rs[at, piece] = rs[at, piece] + pst[stage, core, piece] + pp[slot, piece]
                        sum_copy(rs, at, at + 1, sub).start()

                    @pl.when(s == hops)
                    def _():
                        total = rs[rbase + hops - 1, piece] + pst[stage, core, piece] + pp[slot, piece] + home[piece]
                        if layer + 1 < layers:
                            xb[own + chips, core, piece] = total.astype(jnp.bfloat16)
                            token_copy(own + chips, base + chips, sub).start()
                        else:
                            out[piece] = total.astype(jnp.bfloat16)

            @pl.when(s + 1 < chips)
            def _():
                partial(s + 1)
            return carry

        relay(base, True)
        for copy in expert_loads(layer):
            copy.wait()
        if layer + 1 < layers:
            for copy in expert_loads(layer + 1):
                copy.start()
        if layer == 0:
            for off in range(1, axis_size):
                gate_arrival(off).wait_recv()
        lax.fori_loop(-1, chips, step, 0)
        if layer + 1 < layers:
            mate_copy(own + chips).start()
        for stage in range(2):
            for c in range(width // cols):
                part_copy(stage, base, c).wait_send()

    for off in range(1, axis_size):
        gate_copy(off).wait_send()

    def settle(n, carry):
        layer, s = lax.div(n, chips), lax.rem(n, chips)
        mate_copy(n).wait_send()

        @pl.when(s < hops)
        def _():
            for sub in range(SUBS):
                token_copy(n, n, sub).wait_send()
                sum_copy(first, 0, layer * hops + s, sub).wait_send()
        return carry

    lax.fori_loop(0, layers * chips, settle, 0)
    for off in range(1, groups):
        flag_copy(off).wait()
    any_flag[0] = jnp.max(jnp.max(fbuf[...], axis=0))


def both_layers(axis_size, groups, cid, tok, gt, flag, wg, wu, wd, sg, su, sd):
    layers, depth, cols = wg.shape
    rows, width = tok.shape
    chips = axis_size // 2
    hops = chips - 1
    bf16, f32 = jnp.bfloat16, jnp.float32
    dma = pltpu.SemaphoreType.DMA
    full = layers * chips
    return pl.pallas_call(
        functools.partial(token_kernel, axis_size, groups),
        out_shape=(jax.ShapeDtypeStruct(tok.shape, bf16), jax.ShapeDtypeStruct((1,), flag.dtype)),
        in_specs=[VM, VM, VM] + [ANY] * 6, out_specs=(VM, SM),
        scratch_shapes=[pltpu.VMEM((full, 2, rows, width), bf16), pltpu.VMEM((layers * hops, rows, width), f32),
                        pltpu.VMEM((full, rows, width), f32), pltpu.VMEM((2, 2, rows, width), f32),
                        pltpu.VMEM((layers, rows, width), f32), pltpu.VMEM((rows, width), f32),
                        pltpu.VMEM((axis_size, layers, rows), f32), pltpu.VMEM((groups,) + flag.shape, flag.dtype),
                        pltpu.VMEM((layers, depth, cols), bf16), pltpu.VMEM((layers, depth, cols), bf16),
                        pltpu.VMEM((layers, cols, depth), bf16),
                        pltpu.VMEM((depth, cols), bf16), pltpu.VMEM((depth, cols), bf16), pltpu.VMEM((cols, depth), bf16),
                        dma((3 * layers,)), dma((3,)), dma((axis_size,)), dma((axis_size,)),
                        dma((full, SUBS)), dma((full, SUBS)), dma((full,)), dma((full,)),
                        dma((2, width // cols)), dma((full, width // cols)), dma((layers * hops, SUBS)), dma((layers * hops, SUBS)), dma((groups,)), dma((groups,))],
        compiler_params=pltpu.CompilerParams(collective_id=cid, has_side_effects=True, vmem_limit_bytes=63 * 1024 * 1024),
    )(tok, gt, flag, wg, wu, wd, sg, su, sd)


def solution(mesh):
    def body(tok_in, routes, gate_vals, w_gate, w_up, w_down, sh_gate, sh_up, sh_down, old_map, move_slot, move_expert):
        axis_size = mesh.shape['ep']
        me = lax.axis_index('ep').astype(jnp.int32)[None]
        plan = plan_moves(me, old_map, move_slot, move_expert, axis_size // 2)
        hit = routes[None] == plan[5].T[:, :, None, None]
        gates = jnp.sum(jnp.where(hit, gate_vals[None], 0.0), axis=3)
        tok_out, level = both_layers(axis_size, mesh.shape['replica'], 0, tok_in, gates, plan[4], w_gate[:, 0], w_up[:, 0], w_down[:, 0], sh_gate, sh_up, sh_down)
        placed = new_layout(axis_size, plan, level[0], w_gate, w_up, w_down)
        return (tok_out, *placed)

    weight_spec = P(None, TOKEN_AXES, None, None)
    route_spec = P(None, TOKEN_AXES, None)
    map_spec = P(None, 'replica')
    shared_spec = P(None, None, None)
    tok_spec = P(TOKEN_AXES, None)
    return jax.shard_map(body, mesh=mesh, in_specs=(tok_spec, route_spec, route_spec, weight_spec, weight_spec, weight_spec, shared_spec, shared_spec, shared_spec, map_spec, map_spec, map_spec), out_specs=(tok_spec, weight_spec, weight_spec, weight_spec), check_vma=False)
```

```python
import functools
import jax
import jax.numpy as jnp
from jax import lax
from jax.experimental import pallas as pl
from jax.experimental.pallas import tpu as pltpu
from jax.sharding import PartitionSpec as P

TOKEN_AXES = ('replica', 'ep')
MESH = pl.DeviceIdType.MESH
ANY = pl.BlockSpec(memory_space=pl.ANY)
VM = pl.BlockSpec(memory_space=pltpu.VMEM)
SM = pl.BlockSpec(memory_space=pltpu.SMEM)

CHUNK = 16
HOP_LAG = 5
OUT_LAG = 2
SLOTS = 48
PARTS = 4
FAST_BUSES, FAST_REACH = (4, 5), 6


def sel(pred, a, b):
    return lax.select_n(pred, b, a)


def plan_kernel(chips, me_ref, old_ref, ms_ref, mx_ref, fast_in, fast_out, slow_in, slow_out, level_ref, serve_ref):
    layers, slots = old_ref.shape
    moves = ms_ref.shape[1]
    full = layers * moves
    me = me_ref[0]
    my_core, my_chip = me & 1, lax.shift_right_logical(me, 1)

    def wrap(x):
        return x & (chips - 1) if chips & (chips - 1) == 0 else lax.rem(x, chips)

    for layer in range(layers):
        held = [old_ref[layer, q] for q in range(slots)]
        for q in range(slots):
            again = jnp.bool_(False)
            for p in range(q):
                again = again | (held[p] == held[q])
            serve_ref[layer, q] = jnp.where(again, -1, held[q])
    for ref in (fast_in, slow_in):
        for a in range(ref.shape[0]):
            for b in range(ref.shape[1]):
                ref[a, b] = 0
    for ref in (fast_out, slow_out):
        for a in range(ref.shape[0]):
            ref[a] = 0
    ring = (1 << chips) - 1

    def arc(start, dist, sign):
        run = lax.shift_left(1, dist) - 1
        low = start if sign > 0 else wrap(start - dist + 1 + chips)
        turned = lax.shift_left(run, low)
        return (turned | lax.shift_right_logical(turned, chips)) & ring

    routes = []
    for n in range(full):
        layer, i = divmod(n, moves)
        want, tgt = mx_ref[layer, i], ms_ref[layer, i]
        tgt_chip = lax.shift_right_logical(tgt, 1)
        best_key, src = jnp.int32(1 << 20), jnp.int32(0)
        for q in range(slots):
            fwd = wrap(tgt_chip - q // 2 + chips)
            key = jnp.minimum(fwd, chips - fwd)
            better = (old_ref[layer, q] == want) & (key < best_key)
            best_key = jnp.where(better, key, best_key)
            src = jnp.where(better, q, src)
        start = lax.shift_right_logical(src, 1)
        fwd = wrap(tgt_chip - start + chips)
        dists = (fwd, chips - fwd)
        bits = (arc(start, dists[0], 1), arc(start, dists[1], -1))
        routes.append((src, tgt, fwd == 0, dists, bits))

    def attempt(order, buses):
        used = [[jnp.int32(0)] * buses for _ in range(2)]
        picks, fits = {}, jnp.bool_(True)
        for half in range(2):
            for n in order:
                _, _, near, dists, bits = routes[n]
                found = []
                for lane in range(2):
                    bus = jnp.int32(buses)
                    for b in reversed(range(buses)):
                        bus = jnp.where((used[lane][b] & bits[lane]) == 0, b, bus)
                    found.append(jnp.where(dists[lane] > FAST_REACH, buses, bus))
                second = found[1] * 2 * chips + dists[1] < found[0] * 2 * chips + dists[0]
                bus = jnp.where(second, found[1], found[0])
                fits = fits & (near | (bus < buses))
                for lane in range(2):
                    mine = jnp.logical_not(near) & (second if lane == 1 else jnp.logical_not(second))
                    for b in range(buses):
                        used[lane][b] = used[lane][b] | jnp.where(mine & (bus == b), bits[lane], 0)
                picks[n, half] = (second.astype(jnp.int32), bus)
        return picks, fits

    evens, odds = list(range(0, full, 2)), list(range(1, full, 2))
    straight = list(range(full))
    orders = [straight, straight[::-1], straight[full // 2:] + straight[:full // 2], odds + evens]
    picks, level = attempt(straight, FAST_BUSES[1])
    level = jnp.where(level, 1, 2)
    for order in orders:
        other, fits = attempt(order, FAST_BUSES[0])
        for key in picks:
            picks[key] = tuple(jnp.where(fits, new, old) for new, old in zip(other[key], picks[key]))
        level = jnp.where(fits, 0, level)
    level_ref[...] = jnp.full(level_ref.shape, level, jnp.int32)

    def emit(in_ref, out_ref, lane, bus, dist, n, half, on):
        src, tgt = routes[n][:2]
        piece = 2 * (n // moves) + half

        @pl.when(on & (my_core == lane) & (my_chip == lax.shift_right_logical(src, 1)))
        def _():
            in_ref[bus, 0] = 1
            in_ref[bus, 1] = ((src & 1) != my_core).astype(jnp.int32)
            in_ref[bus, 2] = piece
            in_ref[bus, 3] = dist

        @pl.when(on & (tgt == me))
        def _():
            out_ref[piece] = jnp.where(my_core == lane, 2 + bus, 2 + full + bus)

    for n in range(full):
        src, tgt, near, dists, _ = routes[n]
        for half in range(2):
            lane, bus = picks[n, half]
            ok = jnp.logical_not(near) & (bus < FAST_BUSES[1])
            emit(fast_in, fast_out, lane, bus, jnp.where(lane == 1, dists[1], dists[0]), n, half, ok)
            emit(slow_in, slow_out, half, n, dists[half], n, half, jnp.logical_not(near))

            @pl.when(near & (tgt == me))
            def _():
                fast_out[2 * (n // moves) + half] = 1
                slow_out[2 * (n // moves) + half] = 1


def plan_moves(me, old_map, move_slot, move_expert, chips):
    layers, moves = move_slot.shape
    full = layers * moves
    i32 = jnp.int32
    return pl.pallas_call(
        functools.partial(plan_kernel, chips),
        out_shape=(jax.ShapeDtypeStruct((FAST_BUSES[1], 4), i32), jax.ShapeDtypeStruct((2 * layers,), i32),
                   jax.ShapeDtypeStruct((full, 4), i32), jax.ShapeDtypeStruct((2 * layers,), i32),
                   jax.ShapeDtypeStruct((8, 128), i32), jax.ShapeDtypeStruct(old_map.shape, i32)),
        in_specs=[SM] * 4, out_specs=(SM,) * 4 + (VM, SM),
    )(me, old_map, move_slot, move_expert)


def bus_kernel(axis_size, buses, reach, full, in_tab, out_tab, wg, wu, wd, ng, nu, nd, *scratch):
    owns, pars = scratch[:PARTS], scratch[PARTS:2 * PARTS]
    recv, send, prx, load_sem, dsend, drecv, send_sem, recv_sem, push_sem, prx_sem = scratch[2 * PARTS:]
    me = lax.axis_index('ep')
    core = lax.rem(me, 2)
    step_dir = 2 - 4 * core
    nxt = lax.rem(me + step_dir + axis_size, axis_size)
    prv = lax.rem(me - step_dir + axis_size, axis_size)
    mate = me + 1 - 2 * core
    layers, tall, width = wg.shape[0], wg.shape[1], wg.shape[3]
    low, blocks = wd.shape[1], wd.shape[3] // width
    half_chunks = (2 * tall + blocks * low) // 2
    span = half_chunks // PARTS

    def pieces(part, g, u, d):
        out = []
        for layer in range(layers):
            areas = [(g.at[layer], 0, tall), (u.at[layer], tall, tall)]
            areas += [(d.at[layer, :, :, pl.ds(n * width, width)], 2 * tall + n * low, low) for n in range(blocks)]
            for half in range(2):
                lo = half * half_chunks + part * span
                for ref, at, size in areas:
                    first, last = max(lo, at), min(lo + span, at + size)
                    if first < last:
                        out.append((ref.at[pl.ds(first - at, last - first)], (2 * layer + half) * span + first - lo, last - first))
        return out

    def local_copies(part, refs, out):
        copies = []
        for n, (ref, at, size) in enumerate(pieces(part, *refs)):
            here = owns[part].at[pl.ds(at, size)]
            copies.append(pltpu.make_async_copy(*((here, ref) if out else (ref, here)), load_sem.at[part, n]))
        return copies

    def share(part):
        if part > 0:
            routes = [(owns[part], pars[part], part)]
        else:
            routes = [(ref, pars[0].at[pl.ds(at, size)], PARTS + n) for n, (ref, at, size) in enumerate(pieces(0, wg, wu, wd))]
        return [pltpu.make_async_remote_copy(src, dst, dsend.at[n], drecv.at[n], device_id={'ep': mate}, device_id_type=MESH)
                for src, dst, n in routes]

    def ring_copy(slot):
        return pltpu.make_async_remote_copy(send.at[slot], recv.at[slot], send_sem.at[slot], recv_sem.at[slot],
                                            device_id={'ep': nxt}, device_id_type=MESH)

    def push_copy(slot):
        return pltpu.make_async_remote_copy(recv.at[slot], prx.at[slot], push_sem.at[slot], prx_sem.at[slot],
                                            device_id={'ep': mate}, device_id_type=MESH)

    for copy in local_copies(0, (wg, wu, wd), False):
        copy.start()
    barrier = pltpu.get_barrier_semaphore()
    for peer in (nxt, prv, mate):
        pl.semaphore_signal(barrier, inc=1, device_id={'ep': peer}, device_id_type=MESH)
    pl.semaphore_wait(barrier, 3)
    for copy in share(0):
        copy.start()
    for part in range(PARTS):
        for copy in local_copies(part, (wg, wu, wd), False):
            copy.wait()
        if part > 0:
            share(part)[0].start()
        else:
            for later in range(1, PARTS):
                for copy in local_copies(later, (wg, wu, wd), False):
                    copy.start()

    sends = half_chunks + (reach - 1) * HOP_LAG
    first_out = reach * HOP_LAG
    first_store = first_out + OUT_LAG
    total = first_store + half_chunks
    edges = {0, HOP_LAG, sends, sends + HOP_LAG, first_out, first_out + half_chunks, total}
    edges |= {p * span for p in range(PARTS + 1)} | {first_store + p * span for p in range(PARTS)}
    edges = sorted(edges)

    for begin, end in zip(edges[:-1], edges[1:]):
        lead = min(begin // span, PARTS - 1)
        if begin % span == 0 and begin < half_chunks:
            for copy in share(lead):
                copy.wait()
        done = (begin - first_store) // span
        if begin >= first_store and (begin - first_store) % span == 0 and done > 0:
            for copy in local_copies(done - 1, (ng, nu, nd), True):
                copy.start()

        def step(t, carry, begin=begin, lead=lead, done=done):
            slot = lax.rem(t, SLOTS)
            old_slot = lax.rem(t - HOP_LAG + SLOTS, SLOTS)
            if HOP_LAG <= begin < sends + HOP_LAG:
                ring_copy(old_slot).wait()
            if begin < sends:
                for j in range(buses):
                    pick = t - (reach - in_tab[j, 3]) * HOP_LAG
                    at = in_tab[j, 2] * span
                    late = at + jnp.minimum(jnp.maximum(pick - lead * span, 0), span - 1)
                    mine, theirs = owns[lead][late], pars[lead][late]
                    if lead > 0:
                        early = at + jnp.minimum(jnp.maximum(pick - (lead - 1) * span, 0), span - 1)
                        fresh = pick >= lead * span
                        mine = sel(fresh, mine, owns[lead - 1][early])
                        theirs = sel(fresh, theirs, pars[lead - 1][early])
                    value = sel(in_tab[j, 1] != 0, theirs, mine)
                    if begin >= HOP_LAG:
                        value = sel(in_tab[j, 0] != 0, value, recv[old_slot, j])
                    send[slot, j] = value
                ring_copy(slot).start()
            if first_out <= begin < first_out + half_chunks:
                push_copy(old_slot).start()
            if begin >= first_store:
                k = t - first_store - done * span
                src = lax.rem(t - OUT_LAG - HOP_LAG + SLOTS, SLOTS)
                push_copy(src).wait()
                for piece in range(2 * layers):
                    code = out_tab[piece]
                    at = piece * span + k
                    value = sel(code == 1, pars[done][at], owns[done][at])
                    for j in range(buses):
                        value = sel(code == 2 + j, recv[src, j], value)
                        value = sel(code == 2 + full + j, prx[src, j], value)
                    owns[done][at] = value
            return carry

        lax.fori_loop(begin, end, step, 0)

    for copy in local_copies(PARTS - 1, (ng, nu, nd), True):
        copy.start()
    for part in range(PARTS):
        for copy in local_copies(part, (ng, nu, nd), True):
            copy.wait()


def move_weights(axis_size, buses, reach, full, cid, in_tab, out_tab, *weights):
    cut = [w.reshape(w.shape[0], w.shape[2] // CHUNK, CHUNK, w.shape[3]) for w in weights]
    layers, tall, _, width = cut[0].shape
    low, blocks = cut[2].shape[1], cut[2].shape[3] // width
    bf16 = jnp.bfloat16
    dma = pltpu.SemaphoreType.DMA
    ring = pltpu.VMEM((SLOTS, buses, CHUNK, width), bf16)
    part = pltpu.VMEM((layers * (2 * tall + blocks * low) // PARTS, CHUNK, width), bf16)
    out = pl.pallas_call(
        functools.partial(bus_kernel, axis_size, buses, reach, full),
        out_shape=tuple(jax.ShapeDtypeStruct(w.shape, bf16) for w in cut),
        in_specs=[SM, SM, ANY, ANY, ANY], out_specs=(ANY,) * 3,
        scratch_shapes=[part] * (2 * PARTS) + [ring, ring, ring,
                        dma((PARTS, 4 * layers)), dma((PARTS + 4 * layers,)), dma((PARTS + 4 * layers,)),
                        dma((SLOTS,)), dma((SLOTS,)), dma((SLOTS,)), dma((SLOTS,))],
        compiler_params=pltpu.CompilerParams(collective_id=cid, has_side_effects=True, vmem_limit_bytes=(42 if buses > 5 else 34) * 1024 * 1024),
    )(in_tab, out_tab, *cut)
    return tuple(n.reshape(w.shape) for n, w in zip(out, weights))


def new_layout(axis_size, plan, level, *weights):
    fast_in, fast_out, slow_in, slow_out = plan[:4]
    full = slow_in.shape[0]

    def fast(buses, cid):
        return lambda *w: move_weights(axis_size, buses, FAST_REACH, full, cid, fast_in, fast_out, *w)

    def slow(*w):
        return move_weights(axis_size, full, axis_size // 2 - 1, full, 3, slow_in, slow_out, *w)

    return lax.switch(level, (fast(FAST_BUSES[0], 1), fast(FAST_BUSES[1], 2), slow), *weights)


SUBS = 2


def token_kernel(axis_size, groups, tok, gt, flag, wg, wu, wd, sg, su, sd, out, any_flag,
                 xb, rs, pp, pst, first, home, gbuf, fbuf, eg, eu, ed, hg, hu, hd,
                 w_sem, s_sem, g_send, g_recv, x_send, x_recv, m_send, m_recv, p_send, p_recv, r_send, r_recv, f_send, f_recv):
    me = lax.axis_index('ep')
    core, chip = lax.rem(me, 2), lax.div(me, 2)
    chips = axis_size // 2
    step_dir = 2 - 4 * core
    nxt = lax.rem(me + step_dir + axis_size, axis_size)
    mate = me + 1 - 2 * core
    layers = wg.shape[0]
    rows, width = tok.shape
    hops = chips - 1
    cols = wg.shape[2]

    def shared_loads(layer):
        return [pltpu.make_async_copy(a.at[layer], b, s_sem.at[n]) for n, (a, b) in enumerate(((sg, hg), (su, hu), (sd, hd)))]

    def expert_loads(layer):
        return [pltpu.make_async_copy(a.at[layer], b.at[layer], w_sem.at[3 * layer + n])
                for n, (a, b) in enumerate(((wg, eg), (wu, eu), (wd, ed)))]

    for copy in shared_loads(0) + expert_loads(0):
        copy.start()
    barrier = pltpu.get_barrier_semaphore()
    for off in range(1, axis_size):
        pl.semaphore_signal(barrier, inc=1, device_id={'ep': lax.rem(me + off, axis_size)}, device_id_type=MESH)
    group = lax.axis_index('replica')
    for off in range(1, groups):
        pl.semaphore_signal(barrier, inc=1, device_id={'replica': lax.rem(group + off, groups)}, device_id_type=MESH)
    pl.semaphore_wait(barrier, axis_size + groups - 2)

    def token_copy(src_slot, dst_slot, sub):
        piece = pl.ds(sub * (rows // SUBS), rows // SUBS)
        return pltpu.make_async_remote_copy(xb.at[src_slot, core, piece], xb.at[dst_slot, core, piece],
                                            x_send.at[dst_slot, sub], x_recv.at[dst_slot, sub],
                                            device_id={'ep': nxt}, device_id_type=MESH)

    def mate_copy(slot):
        return pltpu.make_async_remote_copy(xb.at[slot, core], xb.at[slot, core], m_send.at[slot], m_recv.at[slot],
                                            device_id={'ep': mate}, device_id_type=MESH)

    def mate_arrival(slot):
        other = 1 - core
        return pltpu.make_async_remote_copy(xb.at[slot, other], xb.at[slot, other], m_send.at[slot], m_recv.at[slot],
                                            device_id={'ep': mate}, device_id_type=MESH)

    def part_copy(stage, slot, c):
        blk = pl.ds(c * cols, cols)
        return pltpu.make_async_remote_copy(pst.at[stage, 1 - core, :, blk], pp.at[slot, :, blk], p_send.at[stage, c], p_recv.at[slot, c],
                                            device_id={'ep': mate}, device_id_type=MESH)

    def sum_copy(src, at, slot, sub):
        piece = pl.ds(sub * (rows // SUBS), rows // SUBS)
        return pltpu.make_async_remote_copy(src.at[at, piece], rs.at[slot, piece], r_send.at[slot, sub], r_recv.at[slot, sub],
                                            device_id={'ep': nxt}, device_id_type=MESH)

    xb[hops, core] = tok[...]
    for sub in range(SUBS):
        token_copy(hops, 0, sub).start()
    mate_copy(hops).start()

    def gate_copy(off):
        peer = lax.rem(me + off, axis_size)
        return pltpu.make_async_remote_copy(gt.at[peer], gbuf.at[me], g_send.at[off], g_recv.at[off],
                                            device_id={'ep': peer}, device_id_type=MESH)

    def gate_arrival(off):
        peer = lax.rem(me - off + axis_size, axis_size)
        return pltpu.make_async_remote_copy(gt.at[peer], gbuf.at[peer], g_send.at[off], g_recv.at[off],
                                            device_id={'ep': peer}, device_id_type=MESH)

    for off in range(1, axis_size):
        gate_copy(off).start()
    gbuf[me] = gt[me]

    def flag_copy(off):
        peer = lax.rem(group + off, groups)
        return pltpu.make_async_remote_copy(flag, fbuf.at[off], f_send.at[off], f_recv.at[off],
                                            device_id={'replica': peer}, device_id_type=MESH)

    for off in range(1, groups):
        flag_copy(off).start()
    fbuf[0] = flag[...]

    def inner(x, w_gate, w_up):
        gate_proj = jnp.dot(x, w_gate, preferred_element_type=jnp.float32)
        up_proj = jnp.dot(x, w_up, preferred_element_type=jnp.float32)
        return (jax.nn.silu(gate_proj) * up_proj).astype(jnp.bfloat16)

    def spread(src, layer):
        row = gbuf[src, pl.ds(layer, 1), :]
        return jnp.broadcast_to(row, (rows, rows)).T

    for layer in range(layers):
        base = layer * chips
        rbase = layer * hops
        own = base + hops
        for copy in shared_loads(layer):
            copy.wait()
        mine = xb[own, core]
        act = inner(mine, hg[...], hu[...])
        for c in range(width // cols):
            blk = pl.ds(c * cols, cols)
            home[:, blk] = xb[own, core, :, blk].astype(jnp.float32) + jnp.dot(act, hd[:, blk], preferred_element_type=jnp.float32)
        if layer + 1 < layers:
            for copy in shared_loads(layer + 1):
                copy.start()
        def relay(slot, onward):
            for sub in range(SUBS):
                token_copy(slot, slot, sub).wait_recv()

                @pl.when(onward)
                def _():
                    token_copy(slot, slot + 1, sub).start()
            mate_copy(slot).start()

        def partial(s):
            slot, stage = base + s, lax.rem(s, 2)
            mate_arrival(slot).wait_recv()

            @pl.when(s >= 2)
            def _():
                for c in range(width // cols):
                    part_copy(stage, slot, c).wait_send()
            x = xb[slot].reshape(2 * rows, width)
            act = inner(x, eg[layer], eu[layer])

            @pl.when(s + 1 < hops)
            def _():
                relay(slot + 1, s + 2 < hops)
            src_a = 2 * lax.rem(chip - 1 - s + 2 * chips, chips)
            src_b = 2 * lax.rem(chip + 1 + s, chips) + 1
            scale = jnp.concatenate([spread(src_a, layer), spread(src_b, layer)], axis=0)
            scale = jnp.concatenate([scale] * (cols // rows), axis=1)
            for c in range(width // cols):
                blk = pl.ds(c * cols, cols)
                y = jnp.dot(act, ed[layer, :, blk], preferred_element_type=jnp.float32) * scale
                pst[stage, 0, :, blk] = y[:rows]
                pst[stage, 1, :, blk] = y[rows:]
                part_copy(stage, slot, c).start()

        def step(s, carry):
            @pl.when(s >= 0)
            def _():
                slot, stage = base + s, lax.rem(s, 2)
                for c in range(width // cols):
                    part_copy(stage, slot, c).wait_recv()
                for sub in range(SUBS):
                    piece = pl.ds(sub * (rows // SUBS), rows // SUBS)

                    @pl.when(s == 0)
                    def _():
                        first[layer, piece] = pst[stage, core, piece] + pp[slot, piece]
                        sum_copy(first, layer, rbase, sub).start()

                    @pl.when(s > 0)
                    def _():
                        sum_copy(rs, 0, rbase + s - 1, sub).wait_recv()

                    @pl.when((s > 0) & (s < hops))
                    def _():
                        at = rbase + s - 1
                        rs[at, piece] = rs[at, piece] + pst[stage, core, piece] + pp[slot, piece]
                        sum_copy(rs, at, at + 1, sub).start()

                    @pl.when(s == hops)
                    def _():
                        total = rs[rbase + hops - 1, piece] + pst[stage, core, piece] + pp[slot, piece] + home[piece]
                        if layer + 1 < layers:
                            xb[own + chips, core, piece] = total.astype(jnp.bfloat16)
                            token_copy(own + chips, base + chips, sub).start()
                        else:
                            out[piece] = total.astype(jnp.bfloat16)

            @pl.when(s + 1 < chips)
            def _():
                partial(s + 1)
            return carry

        relay(base, True)
        for copy in expert_loads(layer):
            copy.wait()
        if layer + 1 < layers:
            for copy in expert_loads(layer + 1):
                copy.start()
        if layer == 0:
            for off in range(1, axis_size):
                gate_arrival(off).wait_recv()
        lax.fori_loop(-1, chips, step, 0)
        if layer + 1 < layers:
            mate_copy(own + chips).start()
        for stage in range(2):
            for c in range(width // cols):
                part_copy(stage, base, c).wait_send()

    for off in range(1, axis_size):
        gate_copy(off).wait_send()

    def settle(n, carry):
        layer, s = lax.div(n, chips), lax.rem(n, chips)
        mate_copy(n).wait_send()

        @pl.when(s < hops)
        def _():
            for sub in range(SUBS):
                token_copy(n, n, sub).wait_send()
                sum_copy(first, 0, layer * hops + s, sub).wait_send()
        return carry

    lax.fori_loop(0, layers * chips, settle, 0)
    for off in range(1, groups):
        flag_copy(off).wait()
    any_flag[0] = jnp.max(jnp.max(fbuf[...], axis=0))


def both_layers(axis_size, groups, cid, tok, gt, flag, wg, wu, wd, sg, su, sd):
    layers, depth, cols = wg.shape
    rows, width = tok.shape
    chips = axis_size // 2
    hops = chips - 1
    bf16, f32 = jnp.bfloat16, jnp.float32
    dma = pltpu.SemaphoreType.DMA
    full = layers * chips
    return pl.pallas_call(
        functools.partial(token_kernel, axis_size, groups),
        out_shape=(jax.ShapeDtypeStruct(tok.shape, bf16), jax.ShapeDtypeStruct((1,), flag.dtype)),
        in_specs=[VM, VM, VM] + [ANY] * 6, out_specs=(VM, SM),
        scratch_shapes=[pltpu.VMEM((full, 2, rows, width), bf16), pltpu.VMEM((layers * hops, rows, width), f32),
                        pltpu.VMEM((full, rows, width), f32), pltpu.VMEM((2, 2, rows, width), f32),
                        pltpu.VMEM((layers, rows, width), f32), pltpu.VMEM((rows, width), f32),
                        pltpu.VMEM((axis_size, layers, rows), f32), pltpu.VMEM((groups,) + flag.shape, flag.dtype),
                        pltpu.VMEM((layers, depth, cols), bf16), pltpu.VMEM((layers, depth, cols), bf16),
                        pltpu.VMEM((layers, cols, depth), bf16),
                        pltpu.VMEM((depth, cols), bf16), pltpu.VMEM((depth, cols), bf16), pltpu.VMEM((cols, depth), bf16),
                        dma((3 * layers,)), dma((3,)), dma((axis_size,)), dma((axis_size,)),
                        dma((full, SUBS)), dma((full, SUBS)), dma((full,)), dma((full,)),
                        dma((2, width // cols)), dma((full, width // cols)), dma((layers * hops, SUBS)), dma((layers * hops, SUBS)), dma((groups,)), dma((groups,))],
        compiler_params=pltpu.CompilerParams(collective_id=cid, has_side_effects=True, vmem_limit_bytes=63 * 1024 * 1024),
    )(tok, gt, flag, wg, wu, wd, sg, su, sd)


def solution(mesh):
    def body(tok_in, routes, gate_vals, w_gate, w_up, w_down, sh_gate, sh_up, sh_down, old_map, move_slot, move_expert):
        axis_size = mesh.shape['ep']
        me = lax.axis_index('ep').astype(jnp.int32)[None]
        plan = plan_moves(me, old_map, move_slot, move_expert, axis_size // 2)
        hit = routes[None] == plan[5].T[:, :, None, None]
        gates = jnp.sum(jnp.where(hit, gate_vals[None], 0.0), axis=3)
        tok_out, level = both_layers(axis_size, mesh.shape['replica'], 0, tok_in, gates, plan[4], w_gate[:, 0], w_up[:, 0], w_down[:, 0], sh_gate, sh_up, sh_down)
        placed = new_layout(axis_size, plan, level[0], w_gate, w_up, w_down)
        return (tok_out, *placed)

    weight_spec = P(None, TOKEN_AXES, None, None)
    route_spec = P(None, TOKEN_AXES, None)
    map_spec = P(None, 'replica')
    shared_spec = P(None, None, None)
    tok_spec = P(TOKEN_AXES, None)
    return jax.shard_map(body, mesh=mesh, in_specs=(tok_spec, route_spec, route_spec, weight_spec, weight_spec, weight_spec, shared_spec, shared_spec, shared_spec, map_spec, map_spec, map_spec), out_specs=(tok_spec, weight_spec, weight_spec, weight_spec), check_vma=False)
```
